32 devices in a mesh: node: 16 (over z, x, core), local: 2 (over y).
Axes of the slice: x: 2, y: 2, z: 4, core: 2. Of those that a mesh axis runs over, the one named last changes fastest.
Arguments:
- tokens: bfloat16 [2, 16, 7168], P('local', 'node'), may hold values from -6 to 6
- node_ids: int32 [2, 16, 4], P('local', 'node'), may hold values from 0 to 7, all different within a row; in each aligned block of 16 rows (0 to 15, 16 to 31, ..., all dimensions but the last counted through in order) at most 9 rows name the same one
- gates: bfloat16 [2, 16, 8], P('local', 'node'), may hold values from 0.19921875 to 2
- w_in: bfloat16 [32, 3584, 4096], P(('node', 'local')), may hold values from -0.0625 to 0.0625
- w_out: bfloat16 [16, 2048, 7168], P('node', 'local'), may hold values from -0.125 to 0.125
Outputs:
- mixed: bfloat16 [2, 16, 7168], P('local', 'node')
- balance: float32 [16], P('node')
The draws below stay inside these ranges and needn't reach their ends.
Inputs may be any that keep to these rules, and one draw needn't show every extreme that they name: `node_ids`: each token names 4 different nodes. Among the 16 tokens of one index along the first dimension, no node is named by more than 9 tokens, and in every draw, for some index, some node is named by exactly 9 of them.
All inputs are finite; a program needn't handle non-finite values.
Results may differ from the reference program's by a relative error of at most 0.017.
Values may be sent and summed in bfloat16 or wider, within the bound.
A program may use at most 128 MiB of HBM per device.

```python
import math
import jax
import jax.numpy as jnp
import numpy as np
from jax import lax

D = 7168
FF = 2048
NODE_TOP = 4
TOK_DEV = 1
TOP = 8
GROUPS = 8
RECV = 9
FF_DEV = 2048
N_NODE = 16
N_LOCAL = 2


def shard_levels(key, shape, pieces, smallest, top_value):
    factor_of, own = 1.0, jax.random.fold_in(key, 6)
    for dim, blocks in pieces:
        steps = jnp.exp(jax.random.uniform(jax.random.fold_in(own, dim), (blocks,), jnp.float32, smallest / len(pieces), top_value / len(pieces)))
        factor_of = factor_of * jnp.repeat(steps, shape[dim] // blocks).reshape([-1 if axis == dim else 1 for axis in range(len(shape))])
    return factor_of


def routed_block(stream_key, own, number, rows, number_of, top, limit, lean):
    order = jax.random.permutation(stream_key, number_of)
    heavy_load, usual = shares(number_of, rows * top, limit, lean, True), shares(number_of, rows * top, limit, lean, False)
    places = jnp.arange(number_of)

    def named(lengths, rotation):
        used = int((lengths > 0).sum())
        fixed = max(1, used // 4)
        shifted = fixed + (places - fixed + rotation * (used - fixed)) % max(1, number_of - fixed)
        return jnp.zeros((number_of,), jnp.int32).at[order[jnp.where(places < fixed, places, shifted)]].set(jnp.asarray(lengths, jnp.int32))

    lengths = jnp.where(number % 4 == 0, named(heavy_load, number // 4), named(usual, number - number // 4 - 1))
    mixed = jax.random.permutation(jax.random.fold_in(own, 3), number_of)
    donor, taker = mixed[0:number_of // 2 * 2:2], mixed[1:number_of // 2 * 2:2]
    room = jnp.minimum(lengths[donor] - 1, limit - lengths[taker]) // 2
    room = jnp.where((donor == order[0]) | (taker == order[0]) | (lengths[taker] == 0), 0, jnp.maximum(room, 0))
    shifted = jax.random.randint(jax.random.fold_in(own, 4), (number_of // 2,), 0, 1 << 20) % (room + 1)
    lengths = lengths.at[donor].add(-shifted).at[taker].add(shifted)
    members = jnp.searchsorted(jnp.cumsum(lengths), jnp.arange(rows * top), side="right").astype(jnp.int32)
    grid = members.reshape(top, rows).T
    grid = grid[jax.random.permutation(jax.random.fold_in(own, 1), rows)]
    rotation = jax.random.randint(jax.random.fold_in(own, 2), (rows, 1), 0, top)
    return jnp.take_along_axis(grid, (jnp.arange(top)[None, :] + rotation) % top, axis=1)


def shares(number_of, total, reach, lean, full):
    loads = [(1 << 20) // math.isqrt(grade ** lean) + 1 for grade in range(1, number_of + 1)]
    largest = reach if full else min(reach, max(-(-total // number_of), total * loads[0] // sum(loads)))
    least = 1 if total - largest >= number_of - 1 else 0
    given, rest = [largest] + [least] * (number_of - 1), total - largest - least * (number_of - 1)
    while rest > 0:
        free = [i for i in range(1, number_of) if given[i] < largest] or [i for i in range(1, number_of) if given[i] < reach]
        mass, left = sum([loads[i] for i in free]), rest
        for i in free:
            addition = min(reach - given[i], max(1, left * loads[i] // mass), rest)
            given[i] = given[i] + addition
            rest = rest - addition
    return np.array(given)


def gaussian(stream_key, shape, scale, reach, cuts=(), held_as=jnp.bfloat16):
    values = scale * jax.random.normal(stream_key, shape, jnp.float32)
    if cuts:
        values = values * shard_levels(stream_key, shape, cuts, -0.22, 0.18)
    return jnp.clip(values, -reach, reach).astype(held_as)


def setup_inputs(seed: int = 0) -> dict:
    key_of = jax.random.split(jax.random.key(seed), 6)
    tokens = gaussian(key_of[0], (N_LOCAL, N_NODE * TOK_DEV, D), 1.0, 6.0, ((0, 2), (1, 16)))
    node_ids_keys = jax.random.split(jax.random.fold_in(key_of[1], 1), N_LOCAL * (N_NODE * TOK_DEV) // (N_NODE * TOK_DEV))
    node_ids_turns = jax.random.permutation(jax.random.fold_in(key_of[1], 3), N_LOCAL * (N_NODE * TOK_DEV) // (N_NODE * TOK_DEV))
    node_ids = jax.vmap(lambda own, number: routed_block(jax.random.fold_in(key_of[1], 2), own, number, N_NODE * TOK_DEV, GROUPS, NODE_TOP, RECV, 2))(node_ids_keys, node_ids_turns).reshape((N_LOCAL, N_NODE * TOK_DEV, NODE_TOP))
    gates = jnp.clip(jnp.exp(math.log(2.0) - 2.306499 * jax.random.uniform(key_of[2], (N_LOCAL, N_NODE * TOK_DEV, TOP), jnp.float32) ** shard_levels(key_of[2], (N_LOCAL, N_NODE * TOK_DEV, TOP), ((0, 2), (1, 16)), -0.2, 0.2)), 0.19921875, 2.0).astype(jnp.bfloat16)
    w_in = gaussian(key_of[3], (N_NODE * N_LOCAL, D // 2, 2 * FF_DEV), D ** -0.5, 0.0625, ((0, 32),))
    w_out = gaussian(key_of[4], (N_NODE, FF, D), FF ** -0.5, 0.125, ((0, 16), (1, 2)))
    return dict(tokens=tokens, node_ids=node_ids, gates=gates, w_in=w_in, w_out=w_out)


def reference(tokens, node_ids, gates, w_in, w_out):
    count_all = N_LOCAL * N_NODE * TOK_DEV
    flat_tokens = tokens.reshape(count_all, D)
    flat_ids = node_ids.reshape(count_all, NODE_TOP)
    pair_gates = gates.reshape(count_all, NODE_TOP, 2).astype(jnp.float32)
    width = N_LOCAL * RECV
    half = D // 2
    split = N_LOCAL // 2
    ff_dev = FF // split
    block = FF // N_LOCAL
    positions = jnp.arange(count_all, dtype=jnp.int32)

    def one_expert(expert, total):
        expert = jnp.asarray(expert).astype(jnp.int32)
        group = expert // 2
        side = expert % 2
        hits = flat_ids == group
        visits = jnp.any(hits, axis=1)
        chosen = lax.dynamic_index_in_dim(pair_gates, side, 2, keepdims=False)
        weight = jnp.sum(jnp.where(hits, chosen, jnp.float32(0.0)), axis=1)
        order = jnp.cumsum(visits.astype(jnp.int32)) - 1
        target = jnp.where(visits, order, width).astype(jnp.int32)
        picked = jnp.zeros((width,), jnp.int32).at[target].set(positions, mode="drop")
        valid = jnp.arange(width, dtype=jnp.int32) < jnp.sum(visits.astype(jnp.int32))
        rows = flat_tokens[picked]
        row_gate = jnp.where(valid, weight[picked], jnp.float32(0.0))
        inner = lax.dynamic_slice_in_dim(w_in, (expert * N_LOCAL).astype(jnp.int32), N_LOCAL, 0)
        inner = inner.reshape(split, 2, half, 2, ff_dev).transpose(3, 1, 2, 0, 4).reshape(2, D, FF)
        gate_pre = jnp.dot(rows, inner[0], preferred_element_type=jnp.float32)
        up_pre = jnp.dot(rows, inner[1], preferred_element_type=jnp.float32)
        hidden = (row_gate[:, None] * jax.nn.silu(gate_pre) * up_pre).astype(jnp.bfloat16)
        outer = lax.dynamic_index_in_dim(w_out, expert, 0, keepdims=False).reshape(N_LOCAL, block, D)

        def add_block(index, acc):
            index = jnp.asarray(index).astype(jnp.int32)
            piece = lax.dynamic_slice_in_dim(hidden, (index * block).astype(jnp.int32), block, 1)
            weights = lax.dynamic_index_in_dim(outer, index, 0, keepdims=False)
            term = jnp.dot(piece, weights, preferred_element_type=jnp.float32).astype(jnp.bfloat16)
            term = lax.optimization_barrier(term)
            return acc + term.astype(jnp.float32)

        summed = lax.fori_loop(0, N_LOCAL, add_block, jnp.zeros((width, D), jnp.float32))
        node_out = lax.optimization_barrier(summed.astype(jnp.bfloat16)).astype(jnp.float32)
        node_out = jnp.where(valid[:, None], node_out, jnp.float32(0.0))
        return total.at[picked].add(node_out)

    total = lax.fori_loop(0, N_NODE, one_expert, jnp.zeros((count_all, D), jnp.float32))
    mixed = total.astype(jnp.bfloat16).reshape(N_LOCAL, N_NODE * TOK_DEV, D)
    member = flat_ids[:, :, None] == jnp.arange(N_NODE // 2, dtype=jnp.int32)
    group_count = jnp.sum(member.astype(jnp.float32), axis=(0, 1))
    counted = jnp.repeat(group_count, 2)
    gate_total = jnp.sum(jnp.where(member[:, :, :, None], pair_gates[:, :, None, :], jnp.float32(0.0)), axis=(0, 1)).reshape(N_NODE)
    scale = jnp.float32(N_NODE / (2 * NODE_TOP * count_all))
    balance = (counted * scale) * (gate_total * scale)
    return mixed, balance
```

```python
import functools

import jax
import jax.numpy as jnp
from jax import lax
from jax.experimental import pallas as pl
from jax.experimental.pallas import tpu as pltpu
from jax.sharding import PartitionSpec as P

NODE_TOP = 4


def swapped(value, axis, apart):
    mask = 2**apart
    pairs = [(source, source ^ mask) for source in range(lax.axis_size(axis))]
    return lax.ppermute(value, axis, pairs)


def packing(flat_gate, capacity):
    live = flat_gate > 0
    order = jnp.cumsum(live.astype(jnp.int32)) - 1
    wanted = jnp.arange(capacity, dtype=jnp.int32)[:, None]
    return (live[None, :] & (order[None, :] == wanted)).astype(jnp.bfloat16)


def shards(tokens, node_ids, gates, w_in, w_out):
    nodes = lax.axis_size("node")
    local_count = lax.axis_size("local")
    parity = lax.axis_index("local") % 2
    own = tokens[0]
    routes = node_ids[0]
    tok_count = own.shape[0]
    model = own.shape[1]
    half = model // 2
    groups = nodes // 2
    capacity = tok_count * min(nodes, 2 * NODE_TOP + 1)
    slots = nodes * tok_count
    pair_gates = gates[0].astype(jnp.float32).reshape(tok_count, NODE_TOP, 2)
    member = routes[:, :, None] == jnp.arange(groups, dtype=jnp.int32)
    group_visits = jnp.any(member, axis=1)
    row_visits = jnp.repeat(group_visits, 2, axis=1)
    expert_gate = jnp.sum(
        jnp.where(member[:, :, :, None], pair_gates[:, :, None, :], jnp.float32(0.0)), axis=1
    ).reshape(tok_count, nodes)
    gate_out = expert_gate.T.astype(jnp.bfloat16)
    outbound = jnp.where(row_visits.T[:, :, None], own[None], jnp.zeros((), own.dtype))
    arrived, arrived_gate = (
        lax.all_to_all(outbound, "node", split_axis=0, concat_axis=0, tiled=True),
        lax.all_to_all(gate_out, "node", split_axis=0, concat_axis=0, tiled=True),
    )
    flat_gate = arrived_gate.reshape(slots)
    select = packing(flat_gate, capacity)
    packed = jnp.dot(
        select, arrived.reshape(slots, model), preferred_element_type=jnp.float32
    ).astype(jnp.bfloat16)
    packed_gate = jnp.dot(select, flat_gate[:, None], preferred_element_type=jnp.float32)[
        :, 0
    ].astype(jnp.bfloat16)
    outgoing = jnp.tile(
        packed.reshape(capacity, 2, half).transpose(1, 0, 2), (local_count // 2, 1, 1)
    )
    gate_copies = jnp.broadcast_to(packed_gate[None, :], (local_count, capacity))
    parts, gate_parts = (
        lax.all_to_all(outgoing, "local", split_axis=0, concat_axis=0, tiled=True),
        lax.all_to_all(gate_copies, "local", split_axis=0, concat_axis=0, tiled=True),
    )
    my_rows = parts.reshape(local_count * capacity, half)
    row_gate = gate_parts.reshape(local_count * capacity)
    partial_value = jnp.dot(my_rows, w_in[0], preferred_element_type=jnp.float32)
    summed_pre = partial_value + swapped(partial_value, "local", 0)
    ff_dev = w_in.shape[2] // 2
    hidden = (
        row_gate.astype(jnp.float32)[:, None]
        * jax.nn.silu(summed_pre[:, :ff_dev])
        * summed_pre[:, ff_dev:]
    ).astype(jnp.bfloat16)
    block = w_out.shape[1]
    mine = lax.dynamic_slice_in_dim(hidden, parity * block, block, 1)
    expert_rows = lax.psum_scatter(
        jnp.dot(mine, w_out[0], preferred_element_type=jnp.float32).astype(jnp.bfloat16),
        "local",
        scatter_dimension=0,
        tiled=True,
    )
    unpacked = jnp.dot(select.T, expert_rows, preferred_element_type=jnp.float32).astype(
        jnp.bfloat16
    )
    returned = lax.all_to_all(
        unpacked.reshape(nodes, tok_count, model), "node", split_axis=0, concat_axis=0, tiled=True
    )
    mixed = jnp.sum(returned.astype(jnp.float32), axis=0).astype(jnp.bfloat16)[None]
    tokens_all = tok_count * nodes * local_count
    scale = jnp.float32(nodes / (2 * NODE_TOP * tokens_all))
    counted, gate_total = lax.psum(
        (jnp.sum(row_visits.astype(jnp.float32), axis=0), jnp.sum(expert_gate, axis=0)),
        ("node", "local"),
    )
    counted = lax.dynamic_slice_in_dim(counted, lax.axis_index("node"), 1, 0)
    gate_total = lax.dynamic_slice_in_dim(gate_total, lax.axis_index("node"), 1, 0)
    balance = counted * scale * (gate_total * scale)
    return (mixed, balance)


LANES = 128
F32 = jnp.float32
BF16 = jnp.bfloat16
W_IN_PIECES = 1
W_OUT_PIECES = 1
MESH = pl.DeviceIdType.MESH


def body_of_pair(
    sizes,
    tok_hbm, ids_hbm, gate_hbm, win_ref, wout_ref, mix_ref, bal_ref,
    tok_ref, ids_ref, gate_ref, w1, w2, tstage, msg, xbuf, xstage, xmat, ysend, yrecv, pre, hid, acc, asend, arecv, ostage, bsend,
    brecv, fstage,
    in_sem, w1_sem, w2_sem, d_send, d_recv, f_send, f_recv, y_send, y_recv, a_send, a_recv, b_send, b_recv,
):
    nodes, half, ff, block, model = sizes
    node, mine = lax.axis_index("node"), lax.axis_index("local")
    core, chip = lax.rem(node, 2), lax.div(node, 2)
    peers = nodes
    me = chip * 2 + mine
    rows, wide = 2 * peers, xbuf.shape[1]
    sub = half // LANES
    piece = block // W_IN_PIECES
    cols = model // W_OUT_PIECES
    osub = cols // LANES
    opad = bsend.shape[2]
    mate = {"node": 2 * chip + 1 - core, "local": mine}
    twin = {"node": node, "local": 1 - mine}

    def peer(p):
        return {"node": 2 * lax.div(p, 2) + core, "local": lax.rem(p, 2)}

    def w1_copy(i):
        far, j, part = i // (2 * W_IN_PIECES), (i // 2) % W_IN_PIECES, i % 2
        owner = mine if far else 1 - mine
        off = pl.multiple_of(part * ff + owner * block + j * piece, piece)
        return pltpu.make_async_copy(win_ref.at[0, :, pl.ds(off, piece)], w1.at[i], w1_sem.at[i])

    def w2_copy(j):
        return pltpu.make_async_copy(
            wout_ref.at[0, :, pl.ds(j * cols, cols)], w2.at[j], w2_sem.at[j]
        )

    barrier = pltpu.get_barrier_semaphore()

    def greet(k, _):
        pl.semaphore_signal(
            barrier, inc=1, device_id=peer(lax.rem(me + k, peers)), device_id_type=MESH
        )
        return 0

    lax.fori_loop(1, peers, greet, 0)
    pl.semaphore_signal(barrier, inc=1, device_id=mate, device_id_type=MESH)

    inputs = [
        pltpu.make_async_copy(source, target, in_sem.at[i])
        for i, (source, target) in enumerate(
            ((ids_hbm, ids_ref), (gate_hbm, gate_ref), (tok_hbm, tok_ref))
        )
    ]
    for copy in inputs:
        copy.start()
    for i in range(4 * W_IN_PIECES):
        w1_copy(i).start(priority=1)
    for j in range(W_OUT_PIECES):
        w2_copy(j).start(priority=1)
    for copy in inputs:
        copy.wait()

    lane = lax.broadcasted_iota(jnp.int32, (1, LANES), 1)
    ids, gates = ids_ref[0], gate_ref[0].astype(F32)
    weight = jnp.zeros((1, LANES), F32)
    for m in range(NODE_TOP):
        pair = jnp.where(lane % 2 == 0, gates[:, 2 * m : 2 * m + 1], gates[:, 2 * m + 1 : 2 * m + 2])
        weight += jnp.where(lane // 2 == ids[:, m : m + 1], pair, 0.0)
    tstage[...] = jnp.zeros_like(tstage)
    for h in range(2):
        for k in range(sub):
            at = h * half + k * LANES
            tstage[h * wide + k : h * wide + k + 1, :] = tok_ref[0, :, at : at + LANES].astype(F32)
        tstage[h * wide + sub : h * wide + sub + 1, :] = weight
        msg[h] = tstage[h * wide : (h + 1) * wide, :].astype(BF16)
    xbuf[me] = msg[mine]
    ostage[...] = jnp.zeros_like(ostage)

    pl.semaphore_wait(barrier, peers)

    def d_copy(k, p, slot):
        return pltpu.make_async_remote_copy(
            src_ref=msg.at[lax.rem(p, 2)], dst_ref=xbuf.at[slot], send_sem=d_send.at[k],
            recv_sem=d_recv.at[slot], device_id=peer(p), device_id_type=MESH,
        )

    def f_copy(p):
        return pltpu.make_async_remote_copy(
            src_ref=xbuf.at[p], dst_ref=xbuf.at[peers + p], send_sem=f_send.at[p],
            recv_sem=f_recv.at[p], device_id=mate, device_id_type=MESH,
        )

    def send_token(k, _):
        d_copy(k, lax.rem(me + k, peers), me).start()
        return 0

    lax.fori_loop(1, peers, send_token, 0)
    f_copy(me).start()

    def pass_on(k, _):
        p = lax.rem(me + peers - k, peers)
        d_copy(k, p, p).wait_recv()
        f_copy(p).start()
        return 0

    lax.fori_loop(1, peers, pass_on, 0)

    def widen(t, _):
        xstage[pl.ds(pl.multiple_of(t * wide, wide), wide), :] = xbuf[t].astype(F32)
        return 0

    lax.fori_loop(0, peers, widen, 0)

    def widen_far(t, _):
        f_copy(t).wait_recv()
        return widen(t + peers, 0)

    lax.fori_loop(0, peers, widen_far, 0)
    for k in range(sub):
        xmat[:, k * LANES : (k + 1) * LANES] = xstage[pl.ds(k, rows, stride=wide), :].astype(BF16)
    all_gates = xstage[pl.ds(sub, rows, stride=wide), :]
    lanes = lax.broadcasted_iota(jnp.int32, (rows, LANES), 1)
    own_gate = jnp.sum(jnp.where(lanes == node, all_gates, 0.0), axis=1, keepdims=True)

    def y_copy(i):
        return pltpu.make_async_remote_copy(
            src_ref=ysend.at[i], dst_ref=yrecv.at[i], send_sem=y_send.at[i],
            recv_sem=y_recv.at[i], device_id=twin, device_id_type=MESH,
        )

    def w1_wait(i):
        pltpu.make_async_copy(w1.at[i], w1.at[i], w1_sem.at[i]).wait()

    def project_far(i, _):
        w1_wait(i)
        ysend[i] = jnp.dot(xmat[...], w1[i], preferred_element_type=F32).astype(BF16)
        y_copy(i).start()
        return 0

    lax.fori_loop(0, 2 * W_IN_PIECES, project_far, 0)

    def project_own(i, _):
        w1_wait(2 * W_IN_PIECES + i)
        pre[i] = jnp.dot(xmat[...], w1[2 * W_IN_PIECES + i], preferred_element_type=F32)
        return 0

    lax.fori_loop(0, 2 * W_IN_PIECES, project_own, 0)

    def activate(j, _):
        y_copy(2 * j).wait_recv()
        y_copy(2 * j + 1).wait_recv()
        gate_part = pre[2 * j] + yrecv[2 * j].astype(F32)
        up_part = pre[2 * j + 1] + yrecv[2 * j + 1].astype(F32)
        value = own_gate * (gate_part / (1.0 + jnp.exp(-gate_part))) * up_part
        hid[:, pl.ds(pl.multiple_of(j * piece, piece), piece)] = value.astype(BF16)
        return 0

    lax.fori_loop(0, W_IN_PIECES, activate, 0)

    def a_copy(j):
        return pltpu.make_async_remote_copy(
            src_ref=asend.at[j], dst_ref=arecv.at[j], send_sem=a_send.at[j],
            recv_sem=a_recv.at[j], device_id=mate, device_id_type=MESH,
        )

    def b_copy(j, p, slot):
        return pltpu.make_async_remote_copy(
            src_ref=bsend.at[j, p], dst_ref=brecv.at[j, slot], send_sem=b_send.at[j, p],
            recv_sem=b_recv.at[j, slot], device_id=peer(p), device_id_type=MESH,
        )

    def finish(j):
        a_copy(j).wait_recv()
        total = acc[j] + arecv[j].astype(F32)
        for q in range(osub):
            ostage[pl.ds(q, peers, stride=opad), :] = total[:, q * LANES : (q + 1) * LANES]
        for p in range(peers):
            bsend[j, p] = ostage[p * opad : (p + 1) * opad, :].astype(BF16)

        def send_row(k, _):
            b_copy(j, lax.rem(me + k, peers), me).start()
            return 0

        lax.fori_loop(1, peers, send_row, 0)
        brecv[j, me] = bsend[j, me]

    def down(j, _):
        pltpu.make_async_copy(w2.at[j], w2.at[j], w2_sem.at[j]).wait()
        part = jnp.dot(hid[...], w2[j], preferred_element_type=F32)
        asend[j] = part[peers:].astype(BF16)
        acc[j] = part[:peers]
        a_copy(j).start()

        @pl.when(j > 0)
        def _():
            finish(j - 1)

        return 0

    lax.fori_loop(0, W_OUT_PIECES, down, 0)
    finish(W_OUT_PIECES - 1)

    tokens_all = 2.0 * nodes
    scale = nodes / (2 * NODE_TOP * tokens_all)
    count = jnp.sum((own_gate > 0).astype(F32))
    bal_ref[0] = (count * scale) * (jnp.sum(own_gate) * scale)

    for j in range(W_OUT_PIECES):

        def arrive(k, _, j=j):
            p = lax.rem(me + peers - k, peers)
            b_copy(j, p, p).wait_recv()
            return 0

        lax.fori_loop(1, peers, arrive, 0)
        fstage[...] = jnp.sum(brecv[j].astype(F32), axis=0)
        line = jnp.concatenate([fstage[q : q + 1, :] for q in range(osub)], axis=1)
        mix_ref[0, :, j * cols : (j + 1) * cols] = line.astype(BF16)

    def settle(k, _):
        p = lax.rem(me + k, peers)
        d_copy(k, p, me).wait_send()
        for j in range(W_OUT_PIECES):
            b_copy(j, p, me).wait_send()
        return 0

    lax.fori_loop(1, peers, settle, 0)

    def settle_mate(p, _):
        f_copy(p).wait_send()
        return 0

    lax.fori_loop(0, peers, settle_mate, 0)
    for i in range(2 * W_IN_PIECES):
        y_copy(i).wait_send()
    for j in range(W_OUT_PIECES):
        a_copy(j).wait_send()


def fused(tokens, node_ids, gates, w_in, w_out):
    nodes = lax.axis_size("node")
    model, half, ff, block = tokens.shape[2], w_in.shape[1], w_in.shape[2] // 2, w_out.shape[1]
    rows, peers = 2 * nodes, nodes
    sub = half // LANES
    wide = -(-(sub + 1) // 16) * 16
    piece, cols = block // W_IN_PIECES, model // W_OUT_PIECES
    opad = -(-(cols // LANES) // 8) * 8
    sem = pltpu.SemaphoreType.DMA
    vmem = pl.BlockSpec(memory_space=pltpu.VMEM)
    return tuple(pl.pallas_call(
        functools.partial(body_of_pair, (nodes, half, ff, block, model)),
        out_shape=(
            pltpu.VMEM(tokens.shape, BF16),
            pltpu.SMEM((1,), F32),
        ),
        in_specs=[pl.BlockSpec(memory_space=pltpu.HBM)] * 5,
        out_specs=(vmem, pl.BlockSpec(memory_space=pltpu.SMEM)),
        scratch_shapes=[
            pltpu.VMEM(tokens.shape, BF16),
            pltpu.VMEM(node_ids.shape, jnp.int32),
            pltpu.VMEM(gates.shape, BF16),
            pltpu.VMEM((4 * W_IN_PIECES, half, piece), BF16),
            pltpu.VMEM((W_OUT_PIECES, block, cols), BF16),
            pltpu.VMEM((2 * wide, LANES), F32),
            pltpu.VMEM((2, wide, LANES), BF16),
            pltpu.VMEM((rows, wide, LANES), BF16),
            pltpu.VMEM((rows * wide, LANES), F32),
            pltpu.VMEM((rows, half), BF16),
            pltpu.VMEM((2 * W_IN_PIECES, rows, piece), BF16),
            pltpu.VMEM((2 * W_IN_PIECES, rows, piece), BF16),
            pltpu.VMEM((2 * W_IN_PIECES, rows, piece), F32),
            pltpu.VMEM((rows, block), BF16),
            pltpu.VMEM((W_OUT_PIECES, peers, cols), F32),
            pltpu.VMEM((W_OUT_PIECES, peers, cols), BF16),
            pltpu.VMEM((W_OUT_PIECES, peers, cols), BF16),
            pltpu.VMEM((peers * opad, LANES), F32),
            pltpu.VMEM((W_OUT_PIECES, peers, opad, LANES), BF16),
            pltpu.VMEM((W_OUT_PIECES, peers, opad, LANES), BF16),
            pltpu.VMEM((opad, LANES), F32),
            sem((3,)),
            sem((4 * W_IN_PIECES,)),
            sem((W_OUT_PIECES,)),
            sem((peers,)),
            sem((peers,)),
            sem((peers,)),
            sem((peers,)),
            sem((2 * W_IN_PIECES,)),
            sem((2 * W_IN_PIECES,)),
            sem((W_OUT_PIECES,)),
            sem((W_OUT_PIECES,)),
            sem((W_OUT_PIECES, peers)),
            sem((W_OUT_PIECES, peers)),
        ],
        compiler_params=pltpu.CompilerParams(
            collective_id=0, has_side_effects=True, vmem_limit_bytes=60 * 1024 * 1024
        ),
    )(tokens, node_ids, gates, w_in, w_out))


def solution(mesh):
    placed = (
        P("local", "node", None),
        P("local", "node", None),
        P("local", "node", None),
        P(("node", "local"), None, None),
        P("node", "local", None),
    )
    body = fused if mesh.shape["local"] == 2 and mesh.shape["node"] % 2 == 0 else shards
    return jax.shard_map(
        body,
        mesh=mesh,
        in_specs=placed,
        out_specs=(P("local", "node", None), P("node")),
        check_vma=False,
    )
```
